512 devices in a mesh: row: 16 (over z, core), col: 32 (over y, x).
Axes of the slice: x: 4, y: 8, z: 8, core: 2. Of those that a mesh axis runs over, the one named last changes fastest.
Arguments:
- air_flux: bfloat16 [4, 65536, 16, 128], P(None, ('row', 'col')), may hold values from -1 to 3
- air_area: float32 [65536, 128], P(('row', 'col')), may hold values from 0.2 to 2
- sea_area: float32 [65536, 128], P(('row', 'col')), may hold values from 0.2 to 2
- wet_mask: int32 [65536], P(('row', 'col')), may hold values 0 or 1
- intersection_tiles: bfloat16 [32, 128, 128], replicated, may hold values from -0.125 to 0.125
- send_block: int32 [512, 256], P(('row', 'col')), may hold values from 0 to 127
- target_slot: int32 [65536, 16], P(('row', 'col')), may hold values from 0 to 255
- target_tile: int32 [65536, 16], P(('row', 'col')), may hold values from 0 to 31, as said below
Outputs:
- sea_flux: float32 [65536, 16, 128], P(('row', 'col'))
The draws below stay inside these ranges and needn't reach their ends.
Inputs may be any that keep to these rules, and one draw needn't show every extreme that they name: `target_tile`: the 16 entries of a row are distinct.
All inputs are finite; a program needn't handle non-finite values. No bound on the sum of `wet_mask` on one device may be relied on, other than what follows from the above.
Results may differ from the reference program's by a relative error of at most 0.0003.
The reference program's roundings to bfloat16 on the way (of `sent_flux`) count: a program that leaves them out, or rounds other values in their place, can miss the bound.
Values may be sent and summed in bfloat16 or wider, within the bound.
A program may use at most 128 MiB of HBM per device.

```python
import math
import jax
import jax.numpy as jnp
from jax import lax

F = 16
CELLS = 128
K = 16
NTILES = 32
NSTEPS = 4
SB_DEV = 128
CAP = 8
NBLK = 65536
N_ROW = 16
N_COL = 32


def draw_target_tile(key, part):
    scores = jax.random.randint(key, (NBLK, NTILES), 0, 1 << 20) * NTILES + jnp.arange(NTILES, dtype=jnp.int32)[None, :]
    order = jnp.argsort(scores, axis=1, stable=True)
    return order[:, :K].astype(jnp.int32)


def set_ends(result, rng, low, top_value):
    place = [jax.random.randint(jax.random.fold_in(rng, axis), (), 0, length) for axis, length in enumerate(result.shape)]
    main_axis = result.shape.index(max(result.shape))
    next_to = place[:main_axis] + [(place[main_axis] + 1) % result.shape[main_axis]] + place[main_axis + 1:]
    return result.at[tuple(place)].set(low).at[tuple(next_to)].set(top_value)


def level_of(stream_key, extent, shards, least, largest):
    def one(axis_at, shards_of):
        draws = jax.random.uniform(jax.random.fold_in(jax.random.fold_in(stream_key, 6), axis_at), (shards_of,), jnp.float32, least / len(shards), largest / len(shards))
        return jnp.repeat(jnp.exp(draws), extent[axis_at] // shards_of).reshape((-1,) + (1,) * (len(extent) - axis_at - 1))

    level = one(*shards[0])
    for cut in shards[1:]:
        level = level * one(*cut)
    return level


def scatter_about(key, extent, scale, limit, held_as=jnp.bfloat16):
    drawn = jax.random.normal(key, extent, jnp.float32) * scale
    return jnp.minimum(jnp.maximum(drawn, -limit), limit).astype(held_as)


def setup_inputs(seed: int = 0) -> dict:
    keys = jax.random.split(jax.random.key(seed), 9)
    air_flux = jnp.clip(-1.0 + 4.0 * jax.random.uniform(keys[0], (NSTEPS, NBLK, F, CELLS), jnp.float32) ** level_of(keys[0], (NSTEPS, NBLK, F, CELLS), ((1, 512),), -0.2, 0.2), -1.0, 3.0).astype(jnp.bfloat16)
    air_area = jnp.clip(jnp.exp(math.log(2.0) - 2.3025851 * jax.random.uniform(keys[1], (NBLK, CELLS), jnp.float32) ** level_of(keys[1], (NBLK, CELLS), ((0, 512),), -0.2, 0.2)), 0.2, 2.0)
    sea_area = jnp.clip(jnp.exp(math.log(2.0) - 2.3025851 * jax.random.uniform(keys[2], (NBLK, CELLS), jnp.float32) ** level_of(keys[2], (NBLK, CELLS), ((0, 512),), -0.2, 0.2)), 0.2, 2.0)
    wet_mask = set_ends((jax.random.randint(keys[3], (NBLK,), 0, 4) < 3).astype(jnp.int32), jax.random.fold_in(keys[3], 1), 0, 1)
    intersection_tiles = scatter_about(keys[4], (NTILES, CELLS, CELLS), (K * CELLS) ** -0.5, 0.125)
    send_block = set_ends(jax.random.randint(keys[5], (N_ROW * N_COL, N_COL * CAP), 0, SB_DEV), jax.random.fold_in(keys[5], 1), 0, SB_DEV - 1).astype(jnp.int32)
    target_slot = set_ends(jax.random.randint(keys[6], (NBLK, K), 0, N_COL * CAP), jax.random.fold_in(keys[6], 1), 0, (N_COL * CAP) - 1).astype(jnp.int32)
    target_tile = draw_target_tile(jax.random.fold_in(keys[8], 71), 0)
    return {"air_flux": air_flux, "air_area": air_area, "sea_area": sea_area, "wet_mask": wet_mask, "intersection_tiles": intersection_tiles, "send_block": send_block, "target_slot": target_slot, "target_tile": target_tile}


def reference(air_flux, air_area, sea_area, wet_mask, intersection_tiles, send_block, target_slot, target_tile):
    mean_flux = jnp.sum(air_flux, axis=0, dtype=jnp.float32) / NSTEPS
    sent_flux = mean_flux.astype(jnp.bfloat16)
    air_total = jnp.sum(mean_flux * air_area[:, None, :], axis=(0, 2))
    capacity = send_block.shape[1] // N_COL

    def one_device(device):
        band_row = device // N_COL
        column = device % N_COL
        slot_ids = lax.dynamic_slice_in_dim(target_slot, (device * SB_DEV).astype(jnp.int32), SB_DEV, 0)
        tile_ids = lax.dynamic_slice_in_dim(target_tile, (device * SB_DEV).astype(jnp.int32), SB_DEV, 0)
        sender = band_row * N_COL + slot_ids // capacity
        local_block = send_block[sender, column * capacity + slot_ids % capacity]
        source = (sender * SB_DEV + local_block).astype(jnp.int32)
        summed = jnp.zeros((SB_DEV, F, CELLS), jnp.float32)
        for intersection in range(K):
            chosen = sent_flux[source[:, intersection]].astype(jnp.float32)
            weights = intersection_tiles[tile_ids[:, intersection]].astype(jnp.float32)
            summed = summed + jnp.einsum("tfc,tcd->tfd", chosen, weights, precision=lax.Precision.HIGHEST)
        return summed

    raw_flux = lax.map(one_device, jnp.arange(N_ROW * N_COL, dtype=jnp.int32)).reshape(-1, F, CELLS)
    wet_area = wet_mask.astype(jnp.float32)[:, None] * sea_area
    sea_total = jnp.sum(raw_flux * wet_area[:, None, :], axis=(0, 2))
    wet_total = jnp.maximum(jnp.sum(wet_area), 1.0)
    shift = (air_total - sea_total) / wet_total
    return wet_mask.astype(jnp.float32)[:, None, None] * (raw_flux + shift[None, :, None])
```

```python
import functools

import jax
import jax.numpy as jnp
from jax import lax
from jax.experimental import pallas as pl
from jax.experimental.pallas import tpu as pltpu
from jax.sharding import PartitionSpec as P

MESH = pl.DeviceIdType.MESH
WIDE = ("row", "col")
CHUNKS = 4


def peer_order(n_col):
    ny, nx = (8, 4) if n_col == 32 else (n_col, 1)
    ys = sorted(range(ny), key=lambda d: (-min(d, ny - d), d))
    return ny, nx, [(dy, dx) for dx in range(nx) for dy in ys if (dy, dx) != (0, 0)]


def kernel(
    n_row, n_col,
    send_ref, inverse_ref, air_ref, air_area_ref, sea_area_ref, wet_ref, tiles_ref,
    raw_ref, shift_ref,
    air, sent, outbound, received, grouped, part, rows, part_all, cols,
    load_sem, send_sem, recv_sem, row_send, row_recv, col_send, col_recv,
):
    steps, blocks, fields, cells = air.shape
    cap = outbound.shape[0] // n_col
    slots = n_col * cap
    ntiles = tiles_ref.shape[0] // cells
    ny, nx, order = peer_order(n_col)
    me_row = lax.axis_index("row")
    me_col = lax.axis_index("col")
    per = blocks // CHUNKS

    def load(chunk):
        at = pl.ds(chunk * per, per)
        return pltpu.make_async_copy(air_ref.at[:, at], air.at[:, at], load_sem.at[chunk])

    for chunk in range(CHUNKS):
        load(chunk).start()
    barrier = pltpu.get_barrier_semaphore()
    for step in range(1, n_col):
        pl.semaphore_signal(
            barrier, inc=1, device_id={"col": lax.rem(me_col + step, n_col)}, device_id_type=MESH
        )
    for step in range(1, n_row):
        pl.semaphore_signal(
            barrier, inc=1, device_id={"row": lax.rem(me_row + step, n_row)}, device_id_type=MESH
        )

    acc = jnp.zeros((fields, cells), jnp.float32)
    for chunk in range(CHUNKS):
        load(chunk).wait()

        def average(b, acc):
            total = air[0, b].astype(jnp.float32)
            for step in range(1, steps):
                total = total + air[step, b].astype(jnp.float32)
            mean = total * (1.0 / steps)
            sent[b] = mean.astype(jnp.bfloat16)
            return acc + mean * air_area_ref[pl.ds(b, 1), :]

        acc = lax.fori_loop(chunk * per, (chunk + 1) * per, average, acc, unroll=8)

    received[slots] = jnp.zeros((fields, cells), jnp.bfloat16)
    mine = me_col * cap
    pl.semaphore_wait(barrier, n_col + n_row - 2)

    me_y, me_x = me_col // nx, lax.rem(me_col, nx)
    for dy, dx in order:
        peer = lax.rem(me_y + dy, ny) * nx + lax.rem(me_x + dx, nx)
        for j in range(cap):
            outbound[peer * cap + j] = sent[send_ref[0, peer * cap + j]]
        pltpu.make_async_remote_copy(
            src_ref=outbound.at[pl.ds(peer * cap, cap)],
            dst_ref=received.at[pl.ds(mine, cap)],
            send_sem=send_sem,
            recv_sem=recv_sem,
            device_id={"col": peer},
            device_id_type=MESH,
        ).start()
    for j in range(cap):
        received[mine + j] = sent[send_ref[0, mine + j]]

    whole = received.at[pl.ds(0, slots - cap)]
    pltpu.make_async_copy(whole, whole, recv_sem).wait()

    chunk_targets = grouped.shape[0] // fields
    targets = blocks

    def regrid(chunk, sea):
        base = chunk * chunk_targets
        for t in range(chunk_targets):
            for w in range(ntiles):
                slot = inverse_ref[(base + t) * ntiles + w]
                grouped[t * fields:(t + 1) * fields, w * cells:(w + 1) * cells] = received[slot]
        raw = jnp.dot(grouped[...], tiles_ref[...], preferred_element_type=jnp.float32)
        raw = raw.reshape(chunk_targets, fields, cells)
        raw_ref[pl.ds(pl.multiple_of(base, chunk_targets), chunk_targets)] = raw
        at = pl.ds(pl.multiple_of(base, chunk_targets), chunk_targets)
        area = sea_area_ref[at, :] * wet_ref[at, :]
        return sea + jnp.sum(raw * area[:, None, :], axis=0)

    acc = acc - lax.fori_loop(
        0, targets // chunk_targets, regrid, jnp.zeros((fields, cells), jnp.float32)
    )

    lane = lax.broadcasted_iota(jnp.int32, (fields, cells), 1)
    field = lax.broadcasted_iota(jnp.int32, (fields, cells), 0)
    diff = jnp.sum(acc, axis=1, keepdims=True)
    line = jnp.sum(jnp.where(lane == field, diff, 0.0), axis=0, keepdims=True)
    wet = jnp.sum(sea_area_ref[...] * wet_ref[...], axis=0, keepdims=True)
    wet = jnp.sum(wet, axis=1, keepdims=True)
    line = line + jnp.where(lane[:1] == fields, wet, 0.0)

    def gather_sum(line, part, into, n, me, axis, s_sem, r_sem):
        part[0] = line
        into[me] = line
        for step in range(1, n):
            pltpu.make_async_remote_copy(
                src_ref=part.at[0],
                dst_ref=into.at[me],
                send_sem=s_sem,
                recv_sem=r_sem,
                device_id={axis: lax.rem(me + step, n)},
                device_id_type=MESH,
            ).start()
        others = into.at[pl.ds(0, n - 1)]
        pltpu.make_async_copy(others, others, r_sem).wait()
        return jnp.sum(into[...], axis=0)

    line = gather_sum(line, part, rows, n_row, me_row, "row", row_send, row_recv)
    line = gather_sum(line, part_all, cols, n_col, me_col, "col", col_send, col_recv)
    line = jnp.broadcast_to(line, (fields, cells))
    diff = jnp.sum(jnp.where(lane == field, line, 0.0), axis=1, keepdims=True)
    wet = jnp.sum(jnp.where(lane == fields, line, 0.0), axis=1, keepdims=True)
    shift_ref[...] = jnp.broadcast_to(diff / jnp.maximum(wet, 1.0), (fields, cells))

    pltpu.make_async_copy(whole, whole, send_sem).wait()
    others = rows.at[pl.ds(0, n_row - 1)]
    pltpu.make_async_copy(others, others, row_send).wait()
    others = cols.at[pl.ds(0, n_col - 1)]
    pltpu.make_async_copy(others, others, col_send).wait()


def body(n_row, n_col, air_flux, air_area, sea_area, wet_mask, tiles, send_block, slot, tile):
    steps, blocks, fields, cells = air_flux.shape
    ntiles = tiles.shape[0]
    slots = send_block.shape[1]
    ids = jnp.arange(ntiles, dtype=jnp.int32)
    inverse = slots + jnp.sum(
        jnp.where(tile[:, :, None] == ids, slot[:, :, None] - slots, 0), axis=1, dtype=jnp.int32
    )
    wet = wet_mask.astype(jnp.float32)
    wet_wide = jnp.broadcast_to(wet[:, None], (blocks, cells))
    vmem = pl.BlockSpec(memory_space=pltpu.VMEM)
    smem = pl.BlockSpec(memory_space=pltpu.SMEM)
    raw, shift = pl.pallas_call(
        functools.partial(kernel, n_row, n_col),
        out_shape=(
            jax.ShapeDtypeStruct((blocks, fields, cells), jnp.float32),
            jax.ShapeDtypeStruct((fields, cells), jnp.float32),
        ),
        in_specs=[smem, smem, pl.BlockSpec(memory_space=pltpu.HBM), vmem, vmem, vmem, vmem],
        out_specs=(vmem, vmem),
        scratch_shapes=[
            pltpu.VMEM((steps, blocks, fields, cells), jnp.bfloat16),
            pltpu.VMEM((blocks, fields, cells), jnp.bfloat16),
            pltpu.VMEM((slots, fields, cells), jnp.bfloat16),
            pltpu.VMEM((slots + 1, fields, cells), jnp.bfloat16),
            pltpu.VMEM((32 * fields, ntiles * cells), jnp.bfloat16),
            pltpu.VMEM((1, 1, cells), jnp.float32),
            pltpu.VMEM((n_row, 1, cells), jnp.float32),
            pltpu.VMEM((1, 1, cells), jnp.float32),
            pltpu.VMEM((n_col, 1, cells), jnp.float32),
            pltpu.SemaphoreType.DMA((CHUNKS,)),
        ] + [pltpu.SemaphoreType.DMA] * 6,
        compiler_params=pltpu.CompilerParams(
            collective_id=0, has_side_effects=True, vmem_limit_bytes=60 * 1024 * 1024
        ),
    )(
        send_block, inverse.reshape(-1), air_flux, air_area, sea_area, wet_wide,
        tiles.reshape(ntiles * cells, cells),
    )
    return wet[:, None, None] * (raw + shift[None])


def solution(mesh):
    n_row, n_col = mesh.shape["row"], mesh.shape["col"]
    return jax.shard_map(
        functools.partial(body, n_row, n_col),
        mesh=mesh,
        in_specs=(
            P(None, WIDE, None, None), P(WIDE, None), P(WIDE, None), P(WIDE), P(),
            P(WIDE, None), P(WIDE, None), P(WIDE, None),
        ),
        out_specs=P(WIDE, None, None),
        check_vma=False,
    )
```

```python
import functools

import jax
import jax.numpy as jnp
from jax import lax
from jax.experimental import pallas as pl
from jax.experimental.pallas import tpu as pltpu
from jax.sharding import PartitionSpec as P

MESH = pl.DeviceIdType.MESH
WIDE = ("row", "col")
CHUNKS = 4


def peer_order(n_col):
    ny, nx = (8, 4) if n_col == 32 else (n_col, 1)
    ys = sorted(range(ny), key=lambda d: (-min(d, ny - d), d))
    return ny, nx, [(dy, dx) for dx in range(nx) for dy in ys if (dy, dx) != (0, 0)][::-1]


def three_parts(x):
    high = x.astype(jnp.bfloat16)
    rest = x - high.astype(jnp.float32)
    middle = rest.astype(jnp.bfloat16)
    low = (rest - middle.astype(jnp.float32)).astype(jnp.bfloat16)
    return high, middle, low


def kernel(
    n_row, n_col,
    send_ref, slot_ref, tile_ref, air_ref, air_area_ref, sea_area_ref, wet_ref, tiles_ref,
    raw_ref, shift_ref,
    send, slot_of, tile_of, air, air_area, sea_area, wet, tiles,
    inverse_v, inverse, sent, outbound, received, grouped, adjoint, part, rows, part_all, cols,
    small_sem, load_sem, inverse_sem, send_sem, recv_sem, row_send, row_recv, col_send, col_recv,
):
    steps, blocks, fields, cells = air.shape
    cap = outbound.shape[0] // n_col
    slots = n_col * cap
    ntiles = tiles.shape[0]
    ny, nx, order = peer_order(n_col)
    me_row = lax.axis_index("row")
    me_col = lax.axis_index("col")
    per = blocks // CHUNKS

    small = [
        pltpu.make_async_copy(source, target, small_sem.at[i])
        for i, (source, target) in enumerate((
            (send_ref, send), (air_area_ref, air_area), (slot_ref, slot_of), (tile_ref, tile_of),
            (wet_ref, wet), (sea_area_ref, sea_area), (tiles_ref, tiles),
        ))
    ]

    def load(chunk):
        at = pl.ds(chunk * per, per)
        return pltpu.make_async_copy(air_ref.at[:, at], air.at[:, at], load_sem.at[chunk])

    for copy in small[:2]:
        copy.start()
    for chunk in range(CHUNKS):
        load(chunk).start()
    for copy in small[2:]:
        copy.start()
    barrier = pltpu.get_barrier_semaphore()
    for step in range(1, n_col):
        pl.semaphore_signal(
            barrier, inc=1, device_id={"col": lax.rem(me_col + step, n_col)}, device_id_type=MESH
        )
    for step in range(1, n_row):
        pl.semaphore_signal(
            barrier, inc=1, device_id={"row": lax.rem(me_row + step, n_row)}, device_id_type=MESH
        )

    acc = jnp.zeros((fields, cells), jnp.float32)
    for copy in small[:2]:
        copy.wait()
    for chunk in range(CHUNKS):
        load(chunk).wait()

        def average(b, acc):
            total = air[0, b].astype(jnp.float32)
            for step in range(1, steps):
                total = total + air[step, b].astype(jnp.float32)
            mean = total * (1.0 / steps)
            sent[b] = mean.astype(jnp.bfloat16)
            return acc + mean * air_area[pl.ds(b, 1), :]

        acc = lax.fori_loop(chunk * per, (chunk + 1) * per, average, acc, unroll=4)

    for copy in small[2:4]:
        copy.wait()
    tile_id = lax.broadcasted_iota(jnp.int32, (ntiles, blocks), 0)
    found = jnp.full((ntiles, blocks), slots, jnp.int32)
    for k in range(slot_of.shape[0]):
        found = jnp.where(tile_of[k:k + 1, :] == tile_id, slot_of[k:k + 1, :], found)
    inverse_v[...] = found
    received[slots] = jnp.zeros((fields, cells), jnp.bfloat16)
    mine = me_col * cap
    pl.semaphore_wait(barrier, n_col + n_row - 2)

    me_y, me_x = me_col // nx, lax.rem(me_col, nx)
    for i, (dy, dx) in enumerate(order):
        peer = lax.rem(me_y + dy, ny) * nx + lax.rem(me_x + dx, nx)
        for j in range(cap):
            outbound[peer * cap + j] = sent[send[0, peer * cap + j]]
        pltpu.make_async_remote_copy(
            src_ref=outbound.at[pl.ds(peer * cap, cap)],
            dst_ref=received.at[pl.ds(mine, cap)],
            send_sem=send_sem,
            recv_sem=recv_sem.at[i],
            device_id={"col": peer},
            device_id_type=MESH,
        ).start()
    for j in range(cap):
        received[mine + j] = sent[send[0, mine + j]]
    to_scalars = pltpu.make_async_copy(inverse_v, inverse, inverse_sem)
    to_scalars.start()

    for copy in small[4:]:
        copy.wait()
    square = (blocks, blocks)
    on_diagonal = (
        lax.broadcasted_iota(jnp.int32, square, 0) == lax.broadcasted_iota(jnp.int32, square, 1)
    )
    wet_wide = jnp.broadcast_to(wet[...].astype(jnp.float32), square)
    wet_column = jnp.sum(jnp.where(on_diagonal, wet_wide, 0.0), axis=1, keepdims=True)
    wet_area = sea_area[...] * wet_column
    wet_sum = jnp.sum(jnp.sum(wet_area, axis=0, keepdims=True), axis=1, keepdims=True)
    area_parts = jnp.concatenate(three_parts(wet_area), axis=0)
    adjoint[...] = jnp.zeros_like(adjoint)

    def weigh(w, carry):
        back = lax.dot_general(
            area_parts, tiles[w], (((1,), (1,)), ((), ())), preferred_element_type=jnp.float32
        )
        back = back[:blocks] + back[blocks:2 * blocks] + back[2 * blocks:]
        slot_id = lax.broadcasted_iota(jnp.int32, (slots, blocks), 0)
        takes = jnp.where(inverse_v[pl.ds(w, 1), :] == slot_id, 1.0, 0.0).astype(jnp.bfloat16)
        spread = jnp.dot(
            takes, jnp.concatenate(three_parts(back), axis=1), preferred_element_type=jnp.float32
        )
        adjoint[...] += spread[:, :cells] + spread[:, cells:2 * cells] + spread[:, 2 * cells:]
        return carry

    lax.fori_loop(0, ntiles, weigh, 0)
    to_scalars.wait()

    def weighted(first, acc):
        first = pl.multiple_of(first, cap)
        weights = adjoint[pl.ds(first, cap), :]
        for j in range(cap):
            acc = acc - received[first + j].astype(jnp.float32) * weights[j:j + 1]
        return acc

    acc = weighted(mine, acc)
    for i, (dy, dx) in enumerate(order):
        peer = lax.rem(me_y + ny - dy, ny) * nx + lax.rem(me_x + nx - dx, nx)
        arrived = received.at[pl.ds(peer * cap, cap)]
        pltpu.make_async_copy(arrived, arrived, recv_sem.at[i]).wait()
        acc = weighted(peer * cap, acc)

    lane = lax.broadcasted_iota(jnp.int32, (fields, cells), 1)
    field = lax.broadcasted_iota(jnp.int32, (fields, cells), 0)
    diff = jnp.sum(acc, axis=1, keepdims=True)
    line = jnp.sum(jnp.where(lane == field, diff, 0.0), axis=0, keepdims=True)
    line = line + jnp.where(lane[:1] == fields, wet_sum, 0.0)

    def send_line(line, part, into, n, me, axis, s_sem, r_sem):
        part[0] = line
        into[me] = line
        for step in range(1, n):
            pltpu.make_async_remote_copy(
                src_ref=part.at[0],
                dst_ref=into.at[me],
                send_sem=s_sem,
                recv_sem=r_sem,
                device_id={axis: lax.rem(me + step, n)},
                device_id_type=MESH,
            ).start()

    def sum_lines(into, n, r_sem):
        others = into.at[pl.ds(0, n - 1)]
        pltpu.make_async_copy(others, others, r_sem).wait()
        return jnp.sum(into[...], axis=0)

    chunk_targets = blocks // CHUNKS

    def regrid(chunk, carry):
        base = chunk * chunk_targets
        for t in range(chunk_targets):
            for w in range(ntiles):
                slot = inverse[w, base + t]
                grouped[t * fields:(t + 1) * fields, w * cells:(w + 1) * cells] = received[slot]
        raw = jnp.dot(
            grouped[...], tiles[...].reshape(ntiles * cells, cells),
            preferred_element_type=jnp.float32,
        )
        at = pl.ds(pl.multiple_of(base, chunk_targets), chunk_targets)
        raw_ref[at] = raw.reshape(chunk_targets, fields, cells)
        return carry

    send_line(line, part, rows, n_row, me_row, "row", row_send, row_recv)
    lax.fori_loop(0, CHUNKS // 2, regrid, 0)
    line = sum_lines(rows, n_row, row_recv)
    send_line(line, part_all, cols, n_col, me_col, "col", col_send, col_recv)
    lax.fori_loop(CHUNKS // 2, CHUNKS, regrid, 0)
    line = sum_lines(cols, n_col, col_recv)
    line = jnp.broadcast_to(line, (fields, cells))
    diff = jnp.sum(jnp.where(lane == field, line, 0.0), axis=1, keepdims=True)
    wet_all = jnp.sum(jnp.where(lane == fields, line, 0.0), axis=1, keepdims=True)
    shift_ref[...] = jnp.broadcast_to(diff / jnp.maximum(wet_all, 1.0), (fields, cells))

    whole = received.at[pl.ds(0, slots - cap)]
    pltpu.make_async_copy(whole, whole, send_sem).wait()
    others = rows.at[pl.ds(0, n_row - 1)]
    pltpu.make_async_copy(others, others, row_send).wait()
    others = cols.at[pl.ds(0, n_col - 1)]
    pltpu.make_async_copy(others, others, col_send).wait()


def body(n_row, n_col, air_flux, air_area, sea_area, wet_mask, tiles, send_block, slot, tile):
    steps, blocks, fields, cells = air_flux.shape
    ntiles = tiles.shape[0]
    slots = send_block.shape[1]
    kinds = slot.shape[1]
    vmem = pl.BlockSpec(memory_space=pltpu.VMEM)
    raw, shift = pl.pallas_call(
        functools.partial(kernel, n_row, n_col),
        out_shape=(
            jax.ShapeDtypeStruct((blocks, fields, cells), jnp.float32),
            jax.ShapeDtypeStruct((fields, cells), jnp.float32),
        ),
        in_specs=[pl.BlockSpec(memory_space=pltpu.HBM)] * 8,
        out_specs=(vmem, vmem),
        scratch_shapes=[
            pltpu.SMEM((1, slots), jnp.int32),
            pltpu.VMEM((kinds, blocks), jnp.int32),
            pltpu.VMEM((kinds, blocks), jnp.int32),
            pltpu.VMEM((steps, blocks, fields, cells), jnp.bfloat16),
            pltpu.VMEM((blocks, cells), jnp.float32),
            pltpu.VMEM((blocks, cells), jnp.float32),
            pltpu.VMEM((1, blocks), jnp.int32),
            pltpu.VMEM((ntiles, cells, cells), jnp.bfloat16),
            pltpu.VMEM((ntiles, blocks), jnp.int32),
            pltpu.SMEM((ntiles, blocks), jnp.int32),
            pltpu.VMEM((blocks, fields, cells), jnp.bfloat16),
            pltpu.VMEM((slots, fields, cells), jnp.bfloat16),
            pltpu.VMEM((slots + 1, fields, cells), jnp.bfloat16),
            pltpu.VMEM((blocks // CHUNKS * fields, ntiles * cells), jnp.bfloat16),
            pltpu.VMEM((slots, cells), jnp.float32),
            pltpu.VMEM((1, 1, cells), jnp.float32),
            pltpu.VMEM((n_row, 1, cells), jnp.float32),
            pltpu.VMEM((1, 1, cells), jnp.float32),
            pltpu.VMEM((n_col, 1, cells), jnp.float32),
            pltpu.SemaphoreType.DMA((7,)),
            pltpu.SemaphoreType.DMA((CHUNKS,)),
            pltpu.SemaphoreType.DMA,
            pltpu.SemaphoreType.DMA,
            pltpu.SemaphoreType.DMA((n_col - 1,)),
        ] + [pltpu.SemaphoreType.DMA] * 4,
        compiler_params=pltpu.CompilerParams(
            collective_id=0, has_side_effects=True, vmem_limit_bytes=60 * 1024 * 1024
        ),
    )(
        send_block, slot.T, tile.T, air_flux, air_area, sea_area, wet_mask[None], tiles,
    )
    return wet_mask.astype(jnp.float32)[:, None, None] * (raw + shift[None])


def solution(mesh):
    n_row, n_col = mesh.shape["row"], mesh.shape["col"]
    return jax.shard_map(
        functools.partial(body, n_row, n_col),
        mesh=mesh,
        in_specs=(
            P(None, WIDE, None, None), P(WIDE, None), P(WIDE, None), P(WIDE), P(),
            P(WIDE, None), P(WIDE, None), P(WIDE, None),
        ),
        out_specs=P(WIDE, None, None),
        check_vma=False,
    )
```

```python
import functools

import jax
import jax.numpy as jnp
from jax import lax
from jax.experimental import pallas as pl
from jax.experimental.pallas import tpu as pltpu
from jax.sharding import PartitionSpec as P

MESH = pl.DeviceIdType.MESH
WIDE = ("row", "col")
CHUNKS = 4
TARGET_CHUNKS = 4


def peer_order(n_col):
    ny, nx = (8, 4) if n_col == 32 else (n_col // 2, 2)
    ys = sorted(range(ny), key=lambda d: (-min(d, ny - d), d))
    early = [(dy, dx) for dx in range(1, nx) for dy in ys][::-1]
    late = [(dy, 0) for dy in ys if dy]
    return ny, nx, early, late


def three_parts(x):
    high = x.astype(jnp.bfloat16)
    rest = x - high.astype(jnp.float32)
    middle = rest.astype(jnp.bfloat16)
    low = (rest - middle.astype(jnp.float32)).astype(jnp.bfloat16)
    return high, middle, low


def kernel(
    n_row, n_col,
    send_ref, slot_ref, tile_ref, air_ref, air_area_ref, sea_area_ref, wet_ref, tiles_ref,
    raw_ref, shift_ref, wet_out_ref,
    send, slot_of, tile_of, air, air_area, sea_area, wet, tiles,
    inverse_v, inverse, sent, outbound, received, adjoint, returned, part, rows, part_all, cols,
    small_sem, load_sem, inverse_sem, send_sem, recv_sem, back_send, back_recv,
    row_send, row_recv, col_send, col_recv,
):
    steps, blocks, fields, cells = air.shape
    cap = outbound.shape[0] // n_col
    slots = n_col * cap
    ntiles = tiles.shape[0]
    ny, nx, early, late = peer_order(n_col)
    me_row = lax.axis_index("row")
    me_col = lax.axis_index("col")
    per = blocks // CHUNKS

    small = [
        pltpu.make_async_copy(source, target, small_sem.at[i])
        for i, (source, target) in enumerate((
            (send_ref, send), (air_area_ref, air_area), (slot_ref, slot_of), (tile_ref, tile_of),
            (wet_ref, wet), (sea_area_ref, sea_area), (tiles_ref, tiles),
        ))
    ]

    def load(chunk):
        at = pl.ds(chunk * per, per)
        return pltpu.make_async_copy(air_ref.at[:, at], air.at[:, at], load_sem.at[chunk])

    for copy in small[:2]:
        copy.start()
    for chunk in range(CHUNKS):
        load(chunk).start()
    for copy in small[2:]:
        copy.start()
    barrier = pltpu.get_barrier_semaphore()
    for step in range(1, n_col):
        pl.semaphore_signal(
            barrier, inc=1, device_id={"col": lax.rem(me_col + step, n_col)}, device_id_type=MESH
        )
    for step in range(1, n_row):
        pl.semaphore_signal(
            barrier, inc=1, device_id={"row": lax.rem(me_row + step, n_row)}, device_id_type=MESH
        )

    acc = jnp.zeros((fields, cells), jnp.float32)
    for copy in small[:2]:
        copy.wait()
    for chunk in range(CHUNKS):
        load(chunk).wait()

        def average(b, acc):
            total = air[0, b].astype(jnp.float32)
            for step in range(1, steps):
                total = total + air[step, b].astype(jnp.float32)
            mean = total * (1.0 / steps)
            sent[b] = mean.astype(jnp.bfloat16)
            return acc + mean * air_area[pl.ds(b, 1), :]

        acc = lax.fori_loop(chunk * per, (chunk + 1) * per, average, acc, unroll=4)

    for copy in small[2:4]:
        copy.wait()
    tile_id = lax.broadcasted_iota(jnp.int32, (ntiles, blocks), 0)
    found = jnp.full((ntiles, blocks), slots, jnp.int32)
    for k in range(slot_of.shape[0]):
        found = jnp.where(tile_of[k:k + 1, :] == tile_id, slot_of[k:k + 1, :], found)
    inverse_v[...] = found
    received[slots] = jnp.zeros((fields, cells), jnp.bfloat16)
    mine = me_col * cap
    pl.semaphore_wait(barrier, n_col + n_row - 2)

    me_y, me_x = me_col // nx, lax.rem(me_col, nx)

    def ahead(dy, dx):
        return lax.rem(me_y + dy, ny) * nx + lax.rem(me_x + dx, nx)

    def behind(dy, dx):
        return lax.rem(me_y + ny - dy, ny) * nx + lax.rem(me_x + nx - dx, nx)

    def send_blocks(displacements, first):
        for i, (dy, dx) in enumerate(displacements):
            peer = ahead(dy, dx)
            for j in range(cap):
                outbound[peer * cap + j] = sent[send[0, peer * cap + j]]
            pltpu.make_async_remote_copy(
                src_ref=outbound.at[pl.ds(peer * cap, cap)],
                dst_ref=received.at[pl.ds(mine, cap)],
                send_sem=send_sem,
                recv_sem=recv_sem.at[first + i],
                device_id={"col": peer},
                device_id_type=MESH,
            ).start()

    def wait_blocks(displacement, i):
        arrived = received.at[pl.ds(behind(*displacement) * cap, cap)]
        pltpu.make_async_copy(arrived, arrived, recv_sem.at[i]).wait()

    send_blocks(early, 0)
    for j in range(cap):
        received[mine + j] = sent[send[0, mine + j]]
    to_scalars = pltpu.make_async_copy(inverse_v, inverse, inverse_sem)
    to_scalars.start()

    for copy in small[4:]:
        copy.wait()
    square = (blocks, blocks)
    on_diagonal = (
        lax.broadcasted_iota(jnp.int32, square, 0) == lax.broadcasted_iota(jnp.int32, square, 1)
    )
    wet_wide = jnp.broadcast_to(wet[...].astype(jnp.float32), square)
    wet_column = jnp.sum(jnp.where(on_diagonal, wet_wide, 0.0), axis=1, keepdims=True)
    wet_area = sea_area[...] * wet_column
    wet_out_ref[...] = jnp.broadcast_to(wet_column, (blocks, cells))
    wet_sum = jnp.sum(jnp.sum(wet_area, axis=0, keepdims=True), axis=1, keepdims=True)
    area_parts = jnp.concatenate(three_parts(wet_area), axis=0)
    adjoint[...] = jnp.zeros_like(adjoint)

    def weigh(w, carry):
        back = lax.dot_general(
            area_parts, tiles[w], (((1,), (1,)), ((), ())), preferred_element_type=jnp.float32
        )
        back = back[:blocks] + back[blocks:2 * blocks] + back[2 * blocks:]
        slot_id = lax.broadcasted_iota(jnp.int32, (slots, blocks), 0)
        takes = jnp.where(inverse_v[pl.ds(w, 1), :] == slot_id, 1.0, 0.0).astype(jnp.bfloat16)
        spread = jnp.dot(
            takes, jnp.concatenate(three_parts(back), axis=1), preferred_element_type=jnp.float32
        )
        adjoint[...] += spread[:, :cells] + spread[:, cells:2 * cells] + spread[:, 2 * cells:]
        return carry

    lax.fori_loop(0, ntiles, weigh, 0)
    to_scalars.wait()

    for dy, dx in late:
        source = behind(dy, dx)
        pltpu.make_async_remote_copy(
            src_ref=adjoint.at[pl.ds(pl.multiple_of(source * cap, cap), cap)],
            dst_ref=returned.at[pl.ds(pl.multiple_of(mine, cap), cap)],
            send_sem=back_send,
            recv_sem=back_recv,
            device_id={"col": source},
            device_id_type=MESH,
        ).start()
    send_blocks(late, len(early))

    def weighted(values, weights_ref, first, acc):
        first = pl.multiple_of(first, cap)
        weights = weights_ref[pl.ds(first, cap), :]
        for j in range(cap):
            acc = acc - values[first + j].astype(jnp.float32) * weights[j:j + 1]
        return acc

    acc = weighted(received, adjoint, mine, acc)
    for i, displacement in enumerate(early):
        wait_blocks(displacement, i)
        acc = weighted(received, adjoint, behind(*displacement) * cap, acc)
    backs = returned.at[pl.ds(0, cap * len(late))]
    pltpu.make_async_copy(backs, backs, back_recv).wait()
    for displacement in late:
        acc = weighted(outbound, returned, ahead(*displacement) * cap, acc)

    lane = lax.broadcasted_iota(jnp.int32, (fields, cells), 1)
    field = lax.broadcasted_iota(jnp.int32, (fields, cells), 0)
    diff = jnp.sum(acc, axis=1, keepdims=True)
    line = jnp.sum(jnp.where(lane == field, diff, 0.0), axis=0, keepdims=True)
    line = line + jnp.where(lane[:1] == fields, wet_sum, 0.0)

    def send_line(line, part, into, n, me, axis, s_sem, r_sem):
        part[0] = line
        into[me] = line
        for step in range(1, n):
            pltpu.make_async_remote_copy(
                src_ref=part.at[0],
                dst_ref=into.at[me],
                send_sem=s_sem,
                recv_sem=r_sem,
                device_id={axis: lax.rem(me + step, n)},
                device_id_type=MESH,
            ).start()

    def sum_lines(into, n, r_sem):
        others = into.at[pl.ds(0, n - 1)]
        pltpu.make_async_copy(others, others, r_sem).wait()
        return jnp.sum(into[...], axis=0)

    chunk_targets = blocks // TARGET_CHUNKS

    def regrid(chunk):
        base = chunk * chunk_targets
        raw = jnp.zeros((chunk_targets * fields, cells), jnp.float32)
        for w in range(0, ntiles, 2):
            pairs = [
                jnp.concatenate(
                    [received[inverse[w, base + t]], received[inverse[w + 1, base + t]]], axis=1
                )
                for t in range(chunk_targets)
            ]
            raw = raw + jnp.dot(
                jnp.concatenate(pairs, axis=0), tiles[w:w + 2].reshape(2 * cells, cells),
                preferred_element_type=jnp.float32,
            )
        raw_ref[base:base + chunk_targets] = raw.reshape(chunk_targets, fields, cells)

    send_line(line, part, rows, n_row, me_row, "row", row_send, row_recv)
    line = sum_lines(rows, n_row, row_recv)
    send_line(line, part_all, cols, n_col, me_col, "col", col_send, col_recv)
    for i, displacement in enumerate(late):
        wait_blocks(displacement, len(early) + i)
    for chunk in range(TARGET_CHUNKS):
        regrid(chunk)
    line = sum_lines(cols, n_col, col_recv)
    line = jnp.broadcast_to(line, (fields, cells))
    diff = jnp.sum(jnp.where(lane == field, line, 0.0), axis=1, keepdims=True)
    wet_all = jnp.sum(jnp.where(lane == fields, line, 0.0), axis=1, keepdims=True)
    shift_ref[...] = jnp.broadcast_to(diff / jnp.maximum(wet_all, 1.0), (fields, cells))

    whole = received.at[pl.ds(0, slots - cap)]
    pltpu.make_async_copy(whole, whole, send_sem).wait()
    pltpu.make_async_copy(backs, backs, back_send).wait()
    others = rows.at[pl.ds(0, n_row - 1)]
    pltpu.make_async_copy(others, others, row_send).wait()
    others = cols.at[pl.ds(0, n_col - 1)]
    pltpu.make_async_copy(others, others, col_send).wait()


def body(n_row, n_col, air_flux, air_area, sea_area, wet_mask, tiles, send_block, slot, tile):
    steps, blocks, fields, cells = air_flux.shape
    ntiles = tiles.shape[0]
    slots = send_block.shape[1]
    kinds = slot.shape[1]
    vmem = pl.BlockSpec(memory_space=pltpu.VMEM)
    raw, shift, wet = pl.pallas_call(
        functools.partial(kernel, n_row, n_col),
        out_shape=(
            pltpu.VMEM((blocks, fields, cells), jnp.float32),
            pltpu.VMEM((fields, cells), jnp.float32),
            pltpu.VMEM((blocks, cells), jnp.float32),
        ),
        in_specs=[pl.BlockSpec(memory_space=pltpu.HBM)] * 8,
        out_specs=(vmem, vmem, vmem),
        scratch_shapes=[
            pltpu.SMEM((1, slots), jnp.int32),
            pltpu.VMEM((kinds, blocks), jnp.int32),
            pltpu.VMEM((kinds, blocks), jnp.int32),
            pltpu.VMEM((steps, blocks, fields, cells), jnp.bfloat16),
            pltpu.VMEM((blocks, cells), jnp.float32),
            pltpu.VMEM((blocks, cells), jnp.float32),
            pltpu.VMEM((1, blocks), jnp.int32),
            pltpu.VMEM((ntiles, cells, cells), jnp.bfloat16),
            pltpu.VMEM((ntiles, blocks), jnp.int32),
            pltpu.SMEM((ntiles, blocks), jnp.int32),
            pltpu.VMEM((blocks, fields, cells), jnp.bfloat16),
            pltpu.VMEM((slots, fields, cells), jnp.bfloat16),
            pltpu.VMEM((slots + 1, fields, cells), jnp.bfloat16),
            pltpu.VMEM((slots, cells), jnp.float32),
            pltpu.VMEM((slots, cells), jnp.float32),
            pltpu.VMEM((1, 1, cells), jnp.float32),
            pltpu.VMEM((n_row, 1, cells), jnp.float32),
            pltpu.VMEM((1, 1, cells), jnp.float32),
            pltpu.VMEM((n_col, 1, cells), jnp.float32),
            pltpu.SemaphoreType.DMA((7,)),
            pltpu.SemaphoreType.DMA((CHUNKS,)),
            pltpu.SemaphoreType.DMA,
            pltpu.SemaphoreType.DMA,
            pltpu.SemaphoreType.DMA((n_col - 1,)),
        ] + [pltpu.SemaphoreType.DMA] * 6,
        compiler_params=pltpu.CompilerParams(
            collective_id=0, has_side_effects=True, vmem_limit_bytes=55 * 1024 * 1024
        ),
    )(
        send_block, slot.T, tile.T, air_flux, air_area, sea_area, wet_mask[None], tiles,
    )
    return wet[:, None, :] * (raw + shift[None])


def solution(mesh):
    n_row, n_col = mesh.shape["row"], mesh.shape["col"]
    return jax.shard_map(
        functools.partial(body, n_row, n_col),
        mesh=mesh,
        in_specs=(
            P(None, WIDE, None, None), P(WIDE, None), P(WIDE, None), P(WIDE), P(),
            P(WIDE, None), P(WIDE, None), P(WIDE, None),
        ),
        out_specs=P(WIDE, None, None),
        check_vma=False,
    )
```

```python
import functools

import jax
import jax.numpy as jnp
from jax import lax
from jax.experimental import pallas as pl
from jax.experimental.pallas import tpu as pltpu
from jax.sharding import PartitionSpec as P

MESH = pl.DeviceIdType.MESH
WIDE = ("row", "col")
CHUNKS = 4
TILES_A_STEP = 8
HELD = 23
TARGET_CHUNKS = 4


def peer_order(n_col):
    ny, nx = (8, 4) if n_col == 32 else (n_col // 2, 2)
    ys = sorted(range(ny), key=lambda d: (-min(d, ny - d), d))
    every = [(dy, dx) for dx in range(nx) for dy in ys if (dy, dx) != (0, 0)]
    late = [(dy, dx) for dy, dx in every if dx == 0]
    early = [place for place in every[::-1] if place not in late]
    return ny, nx, early, late


def three_parts(x):
    high = x.astype(jnp.bfloat16)
    rest = x - high.astype(jnp.float32)
    middle = rest.astype(jnp.bfloat16)
    low = (rest - middle.astype(jnp.float32)).astype(jnp.bfloat16)
    return high, middle, low


def kernel(
    n_row, n_col,
    send_ref, slot_ref, tile_ref, air_ref, air_area_ref, sea_area_ref, wet_ref, tiles_ref,
    raw_ref, shift_ref, wet_out_ref,
    send, slot_of, tile_of, air, air_area, sea_area, wet, tiles,
    inverse_v, inverse, sent, outbound, received, adjoint, returned, part, rows, part_all, cols,
    small_sem, load_sem, inverse_sem, send_sem, recv_sem, back_send, back_recv,
    row_send, row_recv, col_send, col_recv,
):
    steps, blocks, fields, cells = air.shape
    cap = outbound.shape[0] // n_col
    slots = n_col * cap
    ntiles = tiles.shape[0]
    ny, nx, early, late = peer_order(n_col)
    me_row = lax.axis_index("row")
    me_col = lax.axis_index("col")
    per = blocks // CHUNKS

    small = [
        pltpu.make_async_copy(source, target, small_sem.at[i])
        for i, (source, target) in enumerate((
            (send_ref, send), (air_area_ref, air_area), (slot_ref, slot_of), (tile_ref, tile_of),
            (wet_ref, wet), (sea_area_ref, sea_area), (tiles_ref, tiles),
        ))
    ]

    def load(chunk):
        at = pl.ds(chunk * per, per)
        return pltpu.make_async_copy(air_ref.at[:, at], air.at[:, at], load_sem.at[chunk])

    for copy in small[:2]:
        copy.start()
    for chunk in range(CHUNKS):
        load(chunk).start()
    for copy in small[2:]:
        copy.start()
    barrier = pltpu.get_barrier_semaphore()
    for step in range(1, n_col):
        pl.semaphore_signal(
            barrier, inc=1, device_id={"col": lax.rem(me_col + step, n_col)}, device_id_type=MESH
        )
    for step in range(1, n_row):
        pl.semaphore_signal(
            barrier, inc=1, device_id={"row": lax.rem(me_row + step, n_row)}, device_id_type=MESH
        )

    acc = jnp.zeros((fields, cells), jnp.float32)
    for copy in small[:2]:
        copy.wait()
    for chunk in range(CHUNKS):
        load(chunk).wait()

        def average(b, acc):
            total = air[0, b].astype(jnp.float32)
            for step in range(1, steps):
                total = total + air[step, b].astype(jnp.float32)
            mean = total * (1.0 / steps)
            sent[b] = mean.astype(jnp.bfloat16)
            return acc + mean * air_area[pl.ds(b, 1), :]

        acc = lax.fori_loop(chunk * per, (chunk + 1) * per, average, acc, unroll=4)

    for copy in small[2:4]:
        copy.wait()
    tile_id = lax.broadcasted_iota(jnp.int32, (ntiles, blocks), 0)
    found = jnp.full((ntiles, blocks), slots, jnp.int32)
    for k in range(slot_of.shape[0]):
        found = jnp.where(tile_of[k:k + 1, :] == tile_id, slot_of[k:k + 1, :], found)
    inverse_v[...] = found
    received[slots] = jnp.zeros((fields, cells), jnp.bfloat16)
    mine = me_col * cap
    pl.semaphore_wait(barrier, n_col + n_row - 2)

    me_y, me_x = me_col // nx, lax.rem(me_col, nx)

    def ahead(dy, dx):
        return lax.rem(me_y + dy, ny) * nx + lax.rem(me_x + dx, nx)

    def behind(dy, dx):
        return lax.rem(me_y + ny - dy, ny) * nx + lax.rem(me_x + nx - dx, nx)

    def send_blocks(displacements, first):
        for i, (dy, dx) in enumerate(displacements):
            peer = ahead(dy, dx)
            for j in range(cap):
                outbound[peer * cap + j] = sent[send[0, peer * cap + j]]
            pltpu.make_async_remote_copy(
                src_ref=outbound.at[pl.ds(peer * cap, cap)],
                dst_ref=received.at[pl.ds(mine, cap)],
                send_sem=send_sem,
                recv_sem=recv_sem.at[first + i],
                device_id={"col": peer},
                device_id_type=MESH,
            ).start()

    def wait_blocks(displacement, i):
        arrived = received.at[pl.ds(behind(*displacement) * cap, cap)]
        pltpu.make_async_copy(arrived, arrived, recv_sem.at[i]).wait()

    send_blocks(early, 0)
    for j in range(cap):
        received[mine + j] = sent[send[0, mine + j]]
    to_scalars = pltpu.make_async_copy(inverse_v, inverse, inverse_sem)
    to_scalars.start()

    for copy in small[4:]:
        copy.wait()
    square = (blocks, blocks)
    on_diagonal = (
        lax.broadcasted_iota(jnp.int32, square, 0) == lax.broadcasted_iota(jnp.int32, square, 1)
    )
    wet_wide = jnp.broadcast_to(wet[...].astype(jnp.float32), square)
    wet_column = jnp.sum(jnp.where(on_diagonal, wet_wide, 0.0), axis=1, keepdims=True)
    wet_area = sea_area[...] * wet_column
    wet_out_ref[...] = jnp.broadcast_to(wet_column, (blocks, cells))
    wet_sum = jnp.sum(jnp.sum(wet_area, axis=0, keepdims=True), axis=1, keepdims=True)
    area_parts = jnp.concatenate(three_parts(wet_area), axis=0)
    adjoint[...] = jnp.zeros_like(adjoint)

    slot_id = lax.broadcasted_iota(jnp.int32, (slots, blocks), 0)

    def weigh(step, carry):
        first_tile = step * TILES_A_STEP
        back = lax.dot_general(
            area_parts,
            tiles[pl.ds(first_tile, TILES_A_STEP)].reshape(TILES_A_STEP * cells, cells),
            (((1,), (1,)), ((), ())), preferred_element_type=jnp.float32,
        )
        back = back[:blocks] + back[blocks:2 * blocks] + back[2 * blocks:]
        takes, parts = [], []
        for w in range(TILES_A_STEP):
            taken = inverse_v[pl.ds(first_tile + w, 1), :]
            takes.append(jnp.where(taken == slot_id, 1.0, 0.0).astype(jnp.bfloat16))
            parts.append(
                jnp.concatenate(three_parts(back[:, w * cells:(w + 1) * cells]), axis=1)
            )
        spread = jnp.dot(
            jnp.concatenate(takes, axis=1), jnp.concatenate(parts, axis=0),
            preferred_element_type=jnp.float32,
        )
        adjoint[...] += spread[:, :cells] + spread[:, cells:2 * cells] + spread[:, 2 * cells:]
        return carry

    lax.fori_loop(0, ntiles // TILES_A_STEP, weigh, 0)

    for dy, dx in late:
        source = behind(dy, dx)
        pltpu.make_async_remote_copy(
            src_ref=adjoint.at[pl.ds(pl.multiple_of(source * cap, cap), cap)],
            dst_ref=returned.at[pl.ds(pl.multiple_of(mine, cap), cap)],
            send_sem=back_send,
            recv_sem=back_recv,
            device_id={"col": source},
            device_id_type=MESH,
        ).start()

    def weighted(values, weights_ref, first, acc):
        first = pl.multiple_of(first, cap)
        weights = weights_ref[pl.ds(first, cap), :]
        for j in range(cap):
            acc = acc - values[first + j].astype(jnp.float32) * weights[j:j + 1]
        return acc

    acc = weighted(received, adjoint, mine, acc)
    for i, displacement in enumerate(early):
        if i == HELD * len(early) // 24:
            send_blocks(late, len(early))
        wait_blocks(displacement, i)
        acc = weighted(received, adjoint, behind(*displacement) * cap, acc)
    backs = returned.at[pl.ds(0, cap * len(late))]
    pltpu.make_async_copy(backs, backs, back_recv).wait()
    for displacement in late:
        acc = weighted(outbound, returned, ahead(*displacement) * cap, acc)

    lane = lax.broadcasted_iota(jnp.int32, (fields, cells), 1)
    field = lax.broadcasted_iota(jnp.int32, (fields, cells), 0)
    diff = jnp.sum(acc, axis=1, keepdims=True)
    line = jnp.sum(jnp.where(lane == field, diff, 0.0), axis=0, keepdims=True)
    line = line + jnp.where(lane[:1] == fields, wet_sum, 0.0)

    def send_line(line, part, into, n, me, axis, s_sem, r_sem):
        part[0] = line
        into[me] = line
        for step in range(1, n):
            pltpu.make_async_remote_copy(
                src_ref=part.at[0],
                dst_ref=into.at[me],
                send_sem=s_sem,
                recv_sem=r_sem,
                device_id={axis: lax.rem(me + step, n)},
                device_id_type=MESH,
            ).start()

    def sum_lines(into, n, r_sem):
        others = into.at[pl.ds(0, n - 1)]
        pltpu.make_async_copy(others, others, r_sem).wait()
        return jnp.sum(into[...], axis=0)

    chunk_targets = blocks // TARGET_CHUNKS

    def regrid(chunk):
        base = chunk * chunk_targets
        raw = jnp.zeros((chunk_targets * fields, cells), jnp.float32)
        for w in range(0, ntiles, 2):
            pairs = [
                jnp.concatenate(
                    [received[inverse[w, base + t]], received[inverse[w + 1, base + t]]], axis=1
                )
                for t in range(chunk_targets)
            ]
            raw = raw + jnp.dot(
                jnp.concatenate(pairs, axis=0), tiles[w:w + 2].reshape(2 * cells, cells),
                preferred_element_type=jnp.float32,
            )
        raw_ref[base:base + chunk_targets] = raw.reshape(chunk_targets, fields, cells)

    send_line(line, part, rows, n_row, me_row, "row", row_send, row_recv)
    line = sum_lines(rows, n_row, row_recv)
    send_line(line, part_all, cols, n_col, me_col, "col", col_send, col_recv)
    for i, displacement in enumerate(late):
        wait_blocks(displacement, len(early) + i)
    to_scalars.wait()
    for chunk in range(TARGET_CHUNKS):
        regrid(chunk)
    line = sum_lines(cols, n_col, col_recv)
    line = jnp.broadcast_to(line, (fields, cells))
    diff = jnp.sum(jnp.where(lane == field, line, 0.0), axis=1, keepdims=True)
    wet_all = jnp.sum(jnp.where(lane == fields, line, 0.0), axis=1, keepdims=True)
    shift_ref[...] = jnp.broadcast_to(diff / jnp.maximum(wet_all, 1.0), (fields, cells))

    whole = received.at[pl.ds(0, slots - cap)]
    pltpu.make_async_copy(whole, whole, send_sem).wait()
    pltpu.make_async_copy(backs, backs, back_send).wait()
    others = rows.at[pl.ds(0, n_row - 1)]
    pltpu.make_async_copy(others, others, row_send).wait()
    others = cols.at[pl.ds(0, n_col - 1)]
    pltpu.make_async_copy(others, others, col_send).wait()


def body(n_row, n_col, air_flux, air_area, sea_area, wet_mask, tiles, send_block, slot, tile):
    steps, blocks, fields, cells = air_flux.shape
    ntiles = tiles.shape[0]
    slots = send_block.shape[1]
    kinds = slot.shape[1]
    vmem = pl.BlockSpec(memory_space=pltpu.VMEM)
    raw, shift, wet = pl.pallas_call(
        functools.partial(kernel, n_row, n_col),
        out_shape=(
            pltpu.VMEM((blocks, fields, cells), jnp.float32),
            pltpu.VMEM((fields, cells), jnp.float32),
            pltpu.VMEM((blocks, cells), jnp.float32),
        ),
        in_specs=[pl.BlockSpec(memory_space=pltpu.HBM)] * 8,
        out_specs=(vmem, vmem, vmem),
        scratch_shapes=[
            pltpu.SMEM((1, slots), jnp.int32),
            pltpu.VMEM((kinds, blocks), jnp.int32),
            pltpu.VMEM((kinds, blocks), jnp.int32),
            pltpu.VMEM((steps, blocks, fields, cells), jnp.bfloat16),
            pltpu.VMEM((blocks, cells), jnp.float32),
            pltpu.VMEM((blocks, cells), jnp.float32),
            pltpu.VMEM((1, blocks), jnp.int32),
            pltpu.VMEM((ntiles, cells, cells), jnp.bfloat16),
            pltpu.VMEM((ntiles, blocks), jnp.int32),
            pltpu.SMEM((ntiles, blocks), jnp.int32),
            pltpu.VMEM((blocks, fields, cells), jnp.bfloat16),
            pltpu.VMEM((slots, fields, cells), jnp.bfloat16),
            pltpu.VMEM((slots + 1, fields, cells), jnp.bfloat16),
            pltpu.VMEM((slots, cells), jnp.float32),
            pltpu.VMEM((slots, cells), jnp.float32),
            pltpu.VMEM((1, 1, cells), jnp.float32),
            pltpu.VMEM((n_row, 1, cells), jnp.float32),
            pltpu.VMEM((1, 1, cells), jnp.float32),
            pltpu.VMEM((n_col, 1, cells), jnp.float32),
            pltpu.SemaphoreType.DMA((7,)),
            pltpu.SemaphoreType.DMA((CHUNKS,)),
            pltpu.SemaphoreType.DMA,
            pltpu.SemaphoreType.DMA,
            pltpu.SemaphoreType.DMA((n_col - 1,)),
        ] + [pltpu.SemaphoreType.DMA] * 6,
        compiler_params=pltpu.CompilerParams(
            collective_id=0, has_side_effects=True, vmem_limit_bytes=55 * 1024 * 1024
        ),
    )(
        send_block, slot.T, tile.T, air_flux, air_area, sea_area, wet_mask[None], tiles,
    )
    return wet[:, None, :] * (raw + shift[None])


def solution(mesh):
    n_row, n_col = mesh.shape["row"], mesh.shape["col"]
    return jax.shard_map(
        functools.partial(body, n_row, n_col),
        mesh=mesh,
        in_specs=(
            P(None, WIDE, None, None), P(WIDE, None), P(WIDE, None), P(WIDE), P(),
            P(WIDE, None), P(WIDE, None), P(WIDE, None),
        ),
        out_specs=P(WIDE, None, None),
        check_vma=False,
    )
```

```python
import functools

import jax
import jax.numpy as jnp
from jax import lax
from jax.experimental import pallas as pl
from jax.experimental.pallas import tpu as pltpu
from jax.sharding import PartitionSpec as P

MESH = pl.DeviceIdType.MESH
WIDE = ("row", "col")
CHUNKS = 4
TILES_A_STEP = 8
HELD = 23
TARGET_CHUNKS = 4


def peer_order(n_col):
    ny, nx = (8, 4) if n_col == 32 else (n_col // 2, 2)
    ys = sorted(range(ny), key=lambda d: (-min(d, ny - d), d))
    every = [(dy, dx) for dx in range(nx) for dy in ys if (dy, dx) != (0, 0)]
    late = [(dy, dx) for dy, dx in every[::-1] if dx == 0]
    early = [place for place in every[::-1] if place not in late]
    return ny, nx, early, late


def three_parts(x):
    high = x.astype(jnp.bfloat16)
    rest = x - high.astype(jnp.float32)
    middle = rest.astype(jnp.bfloat16)
    low = (rest - middle.astype(jnp.float32)).astype(jnp.bfloat16)
    return high, middle, low


def kernel(
    n_row, n_col,
    send_ref, slot_ref, tile_ref, air_ref, air_area_ref, sea_area_ref, wet_ref, tiles_ref,
    raw_ref, shift_ref, wet_out_ref,
    send, slot_of, tile_of, air, air_area, sea_area, wet, tiles,
    inverse_v, inverse, sent, outbound, received, adjoint, returned, part, rows, part_all, cols,
    small_sem, load_sem, inverse_sem, send_sem, recv_sem, back_send, back_recv,
    row_send, row_recv, col_send, col_recv,
):
    steps, blocks, fields, cells = air.shape
    cap = outbound.shape[0] // n_col
    slots = n_col * cap
    ntiles = tiles.shape[0]
    ny, nx, early, late = peer_order(n_col)
    me_row = lax.axis_index("row")
    me_col = lax.axis_index("col")
    per = blocks // CHUNKS

    small = [
        pltpu.make_async_copy(source, target, small_sem.at[i])
        for i, (source, target) in enumerate((
            (send_ref, send), (air_area_ref, air_area), (slot_ref, slot_of), (tile_ref, tile_of),
            (wet_ref, wet), (sea_area_ref, sea_area), (tiles_ref, tiles),
        ))
    ]

    def load(chunk):
        at = pl.ds(chunk * per, per)
        return pltpu.make_async_copy(air_ref.at[:, at], air.at[:, at], load_sem.at[chunk])

    for copy in small[:2]:
        copy.start()
    for chunk in range(CHUNKS):
        load(chunk).start()
    for copy in small[2:]:
        copy.start()
    barrier = pltpu.get_barrier_semaphore()
    for step in range(1, n_col):
        pl.semaphore_signal(
            barrier, inc=1, device_id={"col": lax.rem(me_col + step, n_col)}, device_id_type=MESH
        )
    for step in range(1, n_row):
        pl.semaphore_signal(
            barrier, inc=1, device_id={"row": lax.rem(me_row + step, n_row)}, device_id_type=MESH
        )

    acc = jnp.zeros((fields, cells), jnp.float32)
    for copy in small[:2]:
        copy.wait()
    for chunk in range(CHUNKS):
        load(chunk).wait()

        def average(b, acc):
            total = air[0, b].astype(jnp.float32)
            for step in range(1, steps):
                total = total + air[step, b].astype(jnp.float32)
            mean = total * (1.0 / steps)
            sent[b] = mean.astype(jnp.bfloat16)
            return acc + mean * air_area[pl.ds(b, 1), :]

        acc = lax.fori_loop(chunk * per, (chunk + 1) * per, average, acc, unroll=4)

    for copy in small[2:4]:
        copy.wait()
    tile_id = lax.broadcasted_iota(jnp.int32, (ntiles, blocks), 0)
    found = jnp.full((ntiles, blocks), slots, jnp.int32)
    for k in range(slot_of.shape[0]):
        found = jnp.where(tile_of[k:k + 1, :] == tile_id, slot_of[k:k + 1, :], found)
    inverse_v[...] = found
    received[slots] = jnp.zeros((fields, cells), jnp.bfloat16)
    mine = me_col * cap
    pl.semaphore_wait(barrier, n_col + n_row - 2)

    me_y, me_x = me_col // nx, lax.rem(me_col, nx)

    def ahead(dy, dx):
        return lax.rem(me_y + dy, ny) * nx + lax.rem(me_x + dx, nx)

    def behind(dy, dx):
        return lax.rem(me_y + ny - dy, ny) * nx + lax.rem(me_x + nx - dx, nx)

    def send_blocks(displacements, first):
        for i, (dy, dx) in enumerate(displacements):
            peer = ahead(dy, dx)
            for j in range(cap):
                outbound[peer * cap + j] = sent[send[0, peer * cap + j]]
            pltpu.make_async_remote_copy(
                src_ref=outbound.at[pl.ds(peer * cap, cap)],
                dst_ref=received.at[pl.ds(mine, cap)],
                send_sem=send_sem,
                recv_sem=recv_sem.at[first + i],
                device_id={"col": peer},
                device_id_type=MESH,
            ).start()

    def wait_blocks(displacement, i):
        arrived = received.at[pl.ds(behind(*displacement) * cap, cap)]
        pltpu.make_async_copy(arrived, arrived, recv_sem.at[i]).wait()

    send_blocks(early, 0)
    for j in range(cap):
        received[mine + j] = sent[send[0, mine + j]]
    to_scalars = pltpu.make_async_copy(inverse_v, inverse, inverse_sem)
    to_scalars.start()

    for copy in small[4:]:
        copy.wait()
    square = (blocks, blocks)
    on_diagonal = (
        lax.broadcasted_iota(jnp.int32, square, 0) == lax.broadcasted_iota(jnp.int32, square, 1)
    )
    wet_wide = jnp.broadcast_to(wet[...].astype(jnp.float32), square)
    wet_column = jnp.sum(jnp.where(on_diagonal, wet_wide, 0.0), axis=1, keepdims=True)
    wet_area = sea_area[...] * wet_column
    wet_out_ref[...] = jnp.broadcast_to(wet_column, (blocks, cells))
    wet_sum = jnp.sum(jnp.sum(wet_area, axis=0, keepdims=True), axis=1, keepdims=True)
    area_parts = jnp.concatenate(three_parts(wet_area), axis=0)
    adjoint[...] = jnp.zeros_like(adjoint)

    slot_id = lax.broadcasted_iota(jnp.int32, (slots, blocks), 0)

    def weigh(step, carry):
        first_tile = step * TILES_A_STEP
        back = lax.dot_general(
            area_parts,
            tiles[pl.ds(first_tile, TILES_A_STEP)].reshape(TILES_A_STEP * cells, cells),
            (((1,), (1,)), ((), ())), preferred_element_type=jnp.float32,
        )
        back = back[:blocks] + back[blocks:2 * blocks] + back[2 * blocks:]
        takes, parts = [], []
        for w in range(TILES_A_STEP):
            taken = inverse_v[pl.ds(first_tile + w, 1), :]
            takes.append(jnp.where(taken == slot_id, 1.0, 0.0).astype(jnp.bfloat16))
            parts.append(
                jnp.concatenate(three_parts(back[:, w * cells:(w + 1) * cells]), axis=1)
            )
        spread = jnp.dot(
            jnp.concatenate(takes, axis=1), jnp.concatenate(parts, axis=0),
            preferred_element_type=jnp.float32,
        )
        adjoint[...] += spread[:, :cells] + spread[:, cells:2 * cells] + spread[:, 2 * cells:]
        return carry

    lax.fori_loop(0, ntiles // TILES_A_STEP, weigh, 0)

    for dy, dx in late:
        source = behind(dy, dx)
        pltpu.make_async_remote_copy(
            src_ref=adjoint.at[pl.ds(pl.multiple_of(source * cap, cap), cap)],
            dst_ref=returned.at[pl.ds(pl.multiple_of(mine, cap), cap)],
            send_sem=back_send,
            recv_sem=back_recv,
            device_id={"col": source},
            device_id_type=MESH,
        ).start()

    def weighted(values, weights_ref, first, acc):
        first = pl.multiple_of(first, cap)
        weights = weights_ref[pl.ds(first, cap), :]
        for j in range(cap):
            acc = acc - values[first + j].astype(jnp.float32) * weights[j:j + 1]
        return acc

    acc = weighted(received, adjoint, mine, acc)
    for i, displacement in enumerate(early):
        if i == HELD * len(early) // 24:
            send_blocks(late, len(early))
        wait_blocks(displacement, i)
        acc = weighted(received, adjoint, behind(*displacement) * cap, acc)
    backs = returned.at[pl.ds(0, cap * len(late))]
    pltpu.make_async_copy(backs, backs, back_recv).wait()
    for displacement in late:
        acc = weighted(outbound, returned, ahead(*displacement) * cap, acc)

    lane = lax.broadcasted_iota(jnp.int32, (fields, cells), 1)
    field = lax.broadcasted_iota(jnp.int32, (fields, cells), 0)
    diff = jnp.sum(acc, axis=1, keepdims=True)
    line = jnp.sum(jnp.where(lane == field, diff, 0.0), axis=0, keepdims=True)
    line = line + jnp.where(lane[:1] == fields, wet_sum, 0.0)

    def send_line(line, part, into, n, me, axis, s_sem, r_sem):
        part[0] = line
        into[me] = line
        for step in range(1, n):
            pltpu.make_async_remote_copy(
                src_ref=part.at[0],
                dst_ref=into.at[me],
                send_sem=s_sem,
                recv_sem=r_sem,
                device_id={axis: lax.rem(me + step, n)},
                device_id_type=MESH,
            ).start()

    def sum_lines(into, n, r_sem):
        others = into.at[pl.ds(0, n - 1)]
        pltpu.make_async_copy(others, others, r_sem).wait()
        return jnp.sum(into[...], axis=0)

    chunk_targets = blocks // TARGET_CHUNKS

    def regrid(chunk):
        base = chunk * chunk_targets
        raw = jnp.zeros((chunk_targets * fields, cells), jnp.float32)
        for w in range(0, ntiles, 2):
            pairs = [
                jnp.concatenate(
                    [received[inverse[w, base + t]], received[inverse[w + 1, base + t]]], axis=1
                )
                for t in range(chunk_targets)
            ]
            raw = raw + jnp.dot(
                jnp.concatenate(pairs, axis=0), tiles[w:w + 2].reshape(2 * cells, cells),
                preferred_element_type=jnp.float32,
            )
        raw_ref[base:base + chunk_targets] = raw.reshape(chunk_targets, fields, cells)

    send_line(line, part, rows, n_row, me_row, "row", row_send, row_recv)
    line = sum_lines(rows, n_row, row_recv)
    send_line(line, part_all, cols, n_col, me_col, "col", col_send, col_recv)
    for i, displacement in enumerate(late):
        wait_blocks(displacement, len(early) + i)
    to_scalars.wait()
    for chunk in range(TARGET_CHUNKS):
        regrid(chunk)
    line = sum_lines(cols, n_col, col_recv)
    line = jnp.broadcast_to(line, (fields, cells))
    diff = jnp.sum(jnp.where(lane == field, line, 0.0), axis=1, keepdims=True)
    wet_all = jnp.sum(jnp.where(lane == fields, line, 0.0), axis=1, keepdims=True)
    shift_ref[...] = jnp.broadcast_to(diff / jnp.maximum(wet_all, 1.0), (fields, cells))

    whole = received.at[pl.ds(0, slots - cap)]
    pltpu.make_async_copy(whole, whole, send_sem).wait()
    pltpu.make_async_copy(backs, backs, back_send).wait()
    others = rows.at[pl.ds(0, n_row - 1)]
    pltpu.make_async_copy(others, others, row_send).wait()
    others = cols.at[pl.ds(0, n_col - 1)]
    pltpu.make_async_copy(others, others, col_send).wait()


def body(n_row, n_col, air_flux, air_area, sea_area, wet_mask, tiles, send_block, slot, tile):
    steps, blocks, fields, cells = air_flux.shape
    ntiles = tiles.shape[0]
    slots = send_block.shape[1]
    kinds = slot.shape[1]
    vmem = pl.BlockSpec(memory_space=pltpu.VMEM)
    raw, shift, wet = pl.pallas_call(
        functools.partial(kernel, n_row, n_col),
        out_shape=(
            pltpu.VMEM((blocks, fields, cells), jnp.float32),
            pltpu.VMEM((fields, cells), jnp.float32),
            pltpu.VMEM((blocks, cells), jnp.float32),
        ),
        in_specs=[pl.BlockSpec(memory_space=pltpu.HBM)] * 8,
        out_specs=(vmem, vmem, vmem),
        scratch_shapes=[
            pltpu.SMEM((1, slots), jnp.int32),
            pltpu.VMEM((kinds, blocks), jnp.int32),
            pltpu.VMEM((kinds, blocks), jnp.int32),
            pltpu.VMEM((steps, blocks, fields, cells), jnp.bfloat16),
            pltpu.VMEM((blocks, cells), jnp.float32),
            pltpu.VMEM((blocks, cells), jnp.float32),
            pltpu.VMEM((1, blocks), jnp.int32),
            pltpu.VMEM((ntiles, cells, cells), jnp.bfloat16),
            pltpu.VMEM((ntiles, blocks), jnp.int32),
            pltpu.SMEM((ntiles, blocks), jnp.int32),
            pltpu.VMEM((blocks, fields, cells), jnp.bfloat16),
            pltpu.VMEM((slots, fields, cells), jnp.bfloat16),
            pltpu.VMEM((slots + 1, fields, cells), jnp.bfloat16),
            pltpu.VMEM((slots, cells), jnp.float32),
            pltpu.VMEM((slots, cells), jnp.float32),
            pltpu.VMEM((1, 1, cells), jnp.float32),
            pltpu.VMEM((n_row, 1, cells), jnp.float32),
            pltpu.VMEM((1, 1, cells), jnp.float32),
            pltpu.VMEM((n_col, 1, cells), jnp.float32),
            pltpu.SemaphoreType.DMA((7,)),
            pltpu.SemaphoreType.DMA((CHUNKS,)),
            pltpu.SemaphoreType.DMA,
            pltpu.SemaphoreType.DMA,
            pltpu.SemaphoreType.DMA((n_col - 1,)),
        ] + [pltpu.SemaphoreType.DMA] * 6,
        compiler_params=pltpu.CompilerParams(
            collective_id=0, has_side_effects=True, vmem_limit_bytes=55 * 1024 * 1024
        ),
    )(
        send_block, slot.T, tile.T, air_flux, air_area, sea_area, wet_mask[None], tiles,
    )
    return wet[:, None, :] * (raw + shift[None])


def solution(mesh):
    n_row, n_col = mesh.shape["row"], mesh.shape["col"]
    return jax.shard_map(
        functools.partial(body, n_row, n_col),
        mesh=mesh,
        in_specs=(
            P(None, WIDE, None, None), P(WIDE, None), P(WIDE, None), P(WIDE), P(),
            P(WIDE, None), P(WIDE, None), P(WIDE, None),
        ),
        out_specs=P(WIDE, None, None),
        check_vma=False,
    )
```
